32 devices in a mesh: aa: 4 (over y, core), ba: 2 (over x), col: 4 (over z).
Axes of the slice: x: 2, y: 2, z: 4, core: 2. Of those that a mesh axis runs over, the one named last changes fastest.
Arguments:
- right_side: float32 [4, 384, 384, 384], P(None, 'aa', 'ba', 'col'), may hold values from -6 to 6
- shift: float32 [4], replicated, may hold values from 0.5 to 4
Outputs:
- solution: float32 [4, 384, 384, 384], P(None, 'aa', 'ba', 'col')
The draws below stay inside these ranges and needn't reach their ends.
All inputs are finite; a program needn't handle non-finite values.
Results may differ from the reference program's by a relative error of at most 0.0003.
Values sent between devices are 32-bit elements.
A program may use at most 256 MiB of HBM per device.

```python
import math
import jax
import jax.numpy as jnp
from jax import lax

B = 4
NX = 384
NY = 384
NZ = 384


def level_of(key, extent, pieces, low, high):
    def one(dim, shards_of):
        draws = jax.random.uniform(jax.random.fold_in(jax.random.fold_in(key, 6), dim), (shards_of,), jnp.float32, low / len(pieces), high / len(pieces))
        return jnp.repeat(jnp.exp(draws), extent[dim] // shards_of).reshape((-1,) + (1,) * (len(extent) - dim - 1))

    gain = one(*pieces[0])
    for cut in pieces[1:]:
        gain = gain * one(*cut)
    return gain


def gaussian(key, shape, scale, reach, shards=(), held_as=jnp.bfloat16):
    array = jax.random.normal(key, shape, jnp.float32) * scale
    if len(shards) > 0:
        array = level_of(key, shape, shards, -0.22, 0.18) * array
    return jnp.clip(array, min=-reach, max=reach).astype(held_as)


def setup_inputs(seed: int = 0) -> dict:
    arg_keys = jax.random.split(jax.random.key(seed), 3)
    return {
        "right_side": gaussian(arg_keys[0], (B, NX, NY, NZ), 1.0, 6.0, ((1, 4), (2, 2), (3, 4)), jnp.float32),
        "shift": jnp.clip(jax.random.uniform(arg_keys[1], (B,), jnp.float32, 0.5, 4.0), 0.5, 4.0),
    }


def dct_matrix(length):
    freq_ids = jnp.arange(length, dtype=jnp.float32)[:, None]
    cell_ids = jnp.arange(length, dtype=jnp.float32)[None, :]
    weights = jnp.where(freq_ids == 0.0, jnp.float32(math.sqrt(1.0 / length)), jnp.float32(math.sqrt(2.0 / length)))
    return weights * jnp.cos(jnp.float32(math.pi) * freq_ids * (2.0 * cell_ids + 1.0) / (2.0 * length))

def eigen_values(length):
    freq_ids = jnp.arange(length, dtype=jnp.float32)
    return 2.0 - 2.0 * jnp.cos(jnp.float32(math.pi) * freq_ids / length)

def transform(field, matrix, which_dim):
    patterns = ['bnyz,kn->bkyz', 'bxnz,kn->bxkz', 'bxyn,kn->bxyk']
    return jnp.einsum(patterns[which_dim - 1], field, matrix, precision=lax.Precision.HIGHEST)

def reference(right_side, shift):
    along_first = dct_matrix(NX)
    along_second = dct_matrix(NY)
    along_third = dct_matrix(NZ)
    field = transform(right_side, along_first, 1)
    field = transform(field, along_second, 2)
    field = transform(field, along_third, 3)
    denominator = eigen_values(NX)[None, :, None, None] + eigen_values(NY)[None, None, :, None] + eigen_values(NZ)[None, None, None, :] + shift[:, None, None, None]
    field = field / denominator
    field = transform(field, along_second.T, 2)
    field = transform(field, along_third.T, 3)
    field = transform(field, along_first.T, 1)
    return field
```

```python
import math

import jax
import jax.numpy as jnp
from jax import lax
from jax.sharding import PartitionSpec as P

CHUNKS = 1


def dct_matrix(length):
    freq_ids = jnp.arange(length, dtype=jnp.float32)[:, None]
    cell_ids = jnp.arange(length, dtype=jnp.float32)[None, :]
    weights = jnp.where(
        freq_ids == 0.0, jnp.float32(math.sqrt(1.0 / length)), jnp.float32(math.sqrt(2.0 / length))
    )
    return weights * jnp.cos(
        jnp.float32(math.pi) * freq_ids * (2.0 * cell_ids + 1.0) / (2.0 * length)
    )


def eigen_at(global_ids, length):
    return 2.0 - 2.0 * jnp.cos(jnp.float32(math.pi) * global_ids.astype(jnp.float32) / length)


def transform(field, matrix, which_dim):
    patterns = ["bnyz,kn->bkyz", "bxnz,kn->bxkz", "bxyn,kn->bxyk"]
    return jnp.einsum(patterns[which_dim - 1], field, matrix, precision=lax.Precision.HIGH)


def exchange(field, axis, split, concat):
    return lax.all_to_all(field, axis, split_axis=split, concat_axis=concat, tiled=True)


def per_device(right_side, shift):
    nx = right_side.shape[1] * lax.axis_size("aa")
    ny = right_side.shape[2] * lax.axis_size("ba")
    nz = right_side.shape[3] * lax.axis_size("col")
    along_first = dct_matrix(nx)
    along_second = dct_matrix(ny)
    along_third = dct_matrix(nz)
    batch_rows = right_side.shape[0] // lax.axis_size("col")
    shift_part = lax.dynamic_slice_in_dim(shift, lax.axis_index("col") * batch_rows, batch_rows)
    first_part = nx // lax.axis_size("ba")
    first_ids = lax.axis_index("ba") * first_part + jnp.arange(first_part, dtype=jnp.int32)
    chunk = nz // CHUNKS
    third_part = chunk // lax.axis_size("aa")

    field = exchange(right_side, "col", 0, 3)
    parts = []
    for c in range(CHUNKS):
        third_ids = (
            c * chunk
            + lax.axis_index("aa") * third_part
            + jnp.arange(third_part, dtype=jnp.int32)
        )
        part = transform(field, along_third[c * chunk : (c + 1) * chunk], 3)
        part = exchange(part, "aa", 3, 1)
        part = transform(part, along_first, 1)
        part = exchange(part, "ba", 1, 2)
        part = transform(part, along_second, 2)
        denominator = (
            eigen_at(first_ids, nx)[None, :, None, None]
            + eigen_at(jnp.arange(ny, dtype=jnp.int32), ny)[None, None, :, None]
            + eigen_at(third_ids, nz)[None, None, None, :]
            + shift_part[:, None, None, None]
        )
        part = part / denominator
        part = transform(part, along_second.T, 2)
        part = exchange(part, "ba", 2, 1)
        part = transform(part, along_first.T, 1)
        parts.append(exchange(part, "aa", 1, 3))
    field = parts[0] if CHUNKS == 1 else jnp.concatenate(parts, axis=3)
    field = transform(field, along_third.T, 3)
    return exchange(field, "col", 3, 0)


def solution(mesh):
    spec = P(None, "aa", "ba", "col")
    return jax.shard_map(
        per_device, mesh=mesh, in_specs=(spec, P()), out_specs=spec, check_vma=False
    )
```
